32 devices in a mesh: tok: 8 (over z, core), col: 4 (over y, x).
Axes of the slice: x: 2, y: 2, z: 4, core: 2. Of those that a mesh axis runs over, the one named last changes fastest.
Arguments:
- tokens: bfloat16 [8192, 4096], P('tok'), may hold values from -6 to 6
- grads_out: bfloat16 [8192, 8192], P('tok', 'col'), may hold values from -0.0625 to 0.0625
- statistics: float32 [8, 8, 1024, 1024], P('col', 'tok'), as said below
Outputs:
- update: bfloat16 [4096, 8192], P('tok', 'col')
- new_statistics: float32 [8, 8, 1024, 1024], P('col', 'tok')
The draws below stay inside these ranges and needn't reach their ends.
Inputs may be any that keep to these rules, and one draw needn't show every extreme that they name: statistics[j, (2 i + s) + w] holds columns w * 1024 onward of a symmetric positive definite matrix with a positive diagonal.
All inputs are finite; a program needn't handle non-finite values.
Results may differ from the reference program's by a relative error of at most 0.007.
Values may be sent and summed in bfloat16 or wider, within the bound.
A program may use at most 128 MiB of HBM per device.

```python
import math
import jax
import jax.numpy as jnp
from jax import lax

D = 4096
QUERY = 8192
ORDER = 1024
ITERS = 3
TOKENS = 8192
ROW_BLOCKS = 4
COL_BLOCKS = 8
PIECES = 1
N_TOK = 8


def draw_statistics(key, part):
    number_mats = COL_BLOCKS * ROW_BLOCKS * 2

    def one_matrix(seed_key):
        key_base, key_diag = jax.random.split(seed_key)
        base = jax.random.normal(key_base, (ORDER, ORDER), jnp.float32)
        rank_index = jnp.arange(1, ORDER + 1, dtype=jnp.float32)
        exponent = 1.0
        diagonal = jnp.exp(jax.random.uniform(key_diag, (ORDER,), jnp.float32, math.log(0.25 * ORDER), math.log(2.0 * ORDER)))
        strengths = 64.0 * ORDER * jnp.power(rank_index, -exponent)
        weighted = base * strengths[None, :]
        return jnp.dot(weighted, base.T, precision=lax.Precision.HIGHEST) / ORDER + jnp.diag(diagonal)
    matrices = lax.map(one_matrix, jax.random.split(jax.random.fold_in(key, 17), number_mats))
    matrices = matrices.reshape(COL_BLOCKS, ROW_BLOCKS, 2, ORDER, PIECES, ORDER // PIECES)
    return jnp.transpose(matrices, (0, 1, 2, 4, 3, 5)).reshape(COL_BLOCKS, 2 * ROW_BLOCKS * PIECES, ORDER, ORDER // PIECES)


def levels(rng, extent, cuts, smallest, high):
    def one(axis_at, shards_of):
        draws = jax.random.uniform(jax.random.fold_in(jax.random.fold_in(rng, 6), axis_at), (shards_of,), jnp.float32, smallest / len(cuts), high / len(cuts))
        return jnp.repeat(jnp.exp(draws), extent[axis_at] // shards_of).reshape((-1,) + (1,) * (len(extent) - axis_at - 1))

    factor_of = one(*cuts[0])
    for cut in cuts[1:]:
        factor_of = factor_of * one(*cut)
    return factor_of


def centred(own_key, shape, width, limit, cuts=(), kind=jnp.bfloat16):
    level = levels(own_key, shape, cuts, -0.22, 0.18) if cuts else 1.0
    array = jax.random.normal(own_key, shape, jnp.float32) * width * level
    return jnp.minimum(jnp.maximum(array, -limit), limit).astype(kind)


def setup_inputs(seed: int = 0) -> dict:
    splits = jax.random.split(jax.random.key(seed), 4)
    return {
        "tokens": centred(splits[0], (TOKENS, D), 1.0, 6.0, ((0, 8),)),
        "grads_out": centred(splits[1], (TOKENS, QUERY), TOKENS ** -0.5, 0.0625, ((0, 8), (1, 4))),
        "statistics": draw_statistics(jax.random.fold_in(splits[3], 71), 0),
    }


def inverse_root(statistic):
    identity = jnp.eye(statistic.shape[0], dtype=jnp.float32)
    scaling = 2.5 / jnp.sqrt(jnp.sum(statistic * statistic) + 1e-06)
    matrix = scaling * statistic
    factor = (5.0 * identity - matrix) * 0.25
    iterate = jnp.sqrt(jnp.sqrt(scaling)) * factor
    for repeat in range(1, ITERS):
        square = jnp.dot(factor, factor, precision=lax.Precision.HIGHEST)
        fourth = jnp.dot(square, square, precision=lax.Precision.HIGHEST)
        matrix = jnp.dot(fourth, matrix, precision=lax.Precision.HIGHEST)
        factor = (5.0 * identity - matrix) * 0.25
        iterate = jnp.dot(factor, iterate, precision=lax.Precision.HIGHEST)
    return iterate

def reference(tokens, grads_out, statistics):
    pieces = N_TOK // (2 * ROW_BLOCKS)
    assembled = statistics.reshape(COL_BLOCKS, ROW_BLOCKS, 2, pieces, ORDER, ORDER // pieces)
    assembled = jnp.transpose(assembled, (0, 1, 2, 4, 3, 5)).reshape(COL_BLOCKS, ROW_BLOCKS, 2, ORDER, ORDER)
    scale_factor = math.sqrt(ORDER)

    def one_column(column_index):
        columns = lax.dynamic_slice_in_dim(grads_out, column_index * ORDER, ORDER, 1)
        gradient = lax.dot_general(tokens, columns, (((0,), (0,)), ((), ())), preferred_element_type=jnp.float32)
        grad_blocks = gradient.astype(jnp.bfloat16).reshape(ROW_BLOCKS, ORDER, ORDER)
        previous = lax.dynamic_index_in_dim(assembled, column_index, 0, keepdims=False)

        def one_block(inputs_pair):
            grad_block, old_stats = inputs_pair
            left_stat = old_stats[0] + jnp.dot(grad_block, grad_block.T, preferred_element_type=jnp.float32)
            right_stat = old_stats[1] + jnp.dot(grad_block.T, grad_block, preferred_element_type=jnp.float32)
            left_root = inverse_root(left_stat).astype(jnp.bfloat16)
            right_root = inverse_root(right_stat).astype(jnp.bfloat16)
            mixed_rows = jnp.dot(left_root, grad_block, preferred_element_type=jnp.float32).astype(jnp.bfloat16)
            update = (jnp.dot(mixed_rows, right_root, preferred_element_type=jnp.float32) * scale_factor).astype(jnp.bfloat16)
            return (update, jnp.stack([left_stat, right_stat]))
        return lax.map(one_block, (grad_blocks, previous))
    updates, fresh_stats = lax.map(one_column, jnp.arange(COL_BLOCKS, dtype=jnp.int32))
    update = jnp.transpose(updates, (1, 2, 0, 3)).reshape(ROW_BLOCKS * ORDER, COL_BLOCKS * ORDER)
    fresh_stats = fresh_stats.reshape(COL_BLOCKS, ROW_BLOCKS, 2, ORDER, pieces, ORDER // pieces)
    fresh_stats = jnp.transpose(fresh_stats, (0, 1, 2, 4, 3, 5)).reshape(COL_BLOCKS, ROW_BLOCKS * 2 * pieces, ORDER, ORDER // pieces)
    return (update, fresh_stats)
```

```python
import math

import jax
import jax.numpy as jnp
from jax import lax
from jax.sharding import PartitionSpec as P

ITERS = 3


def swapped(block, axis, bit):
    count = lax.axis_size(axis)
    route = []
    for low in range(count):
        high = low | 1 << bit
        if high != low and high < count:
            route += [(low, high), (high, low)]
    return lax.ppermute(block, axis, route)


def as_sent(array):
    return jax.tree.map(lambda a: a.astype(jnp.bfloat16) if a.dtype == jnp.float32 else a, array)


def doubling(values, levels, device, axis_dim, partner):
    for level_bit in range(levels):
        partner_part = partner(values, level_bit)
        low_side = device // 2**level_bit % 2 == 0
        values = jnp.where(
            low_side,
            jnp.concatenate([values, partner_part], axis_dim),
            jnp.concatenate([partner_part, values], axis_dim),
        )
    return values


def product(left_side, right_side):
    return jnp.einsum("bij,bjk->bik", left_side, right_side, precision=lax.Precision.HIGHEST)


def in_pieces(tokens, grads_out, statistics):
    device = lax.axis_index("tok")
    blocks = statistics.shape[0]
    order_size = statistics.shape[2]
    piece_width = statistics.shape[3]
    pieces = order_size // piece_width
    levels = pieces.bit_length() - 1
    rows_dev = tokens.shape[1] // lax.axis_size("tok")
    side_bit = device // pieces % 2
    column = device % pieces
    slab_index = device % (2 * pieces)

    def columns_of(values):
        return lax.dynamic_slice_in_dim(values, column * piece_width, piece_width, 2)

    owned = lax.psum_scatter(
        lax.dot_general(
            tokens, grads_out, (((0,), (0,)), ((), ())), preferred_element_type=jnp.float32
        ),
        "tok",
        scatter_dimension=0,
        tiled=True,
    ).astype(jnp.bfloat16)
    gradient = doubling(
        owned, levels + 1, device, 0, lambda portion, level_bit: swapped(portion, "tok", level_bit)
    )
    grad_cube = gradient.reshape(order_size, blocks, order_size)
    forward = jnp.transpose(grad_cube, (1, 0, 2))
    backward = jnp.transpose(grad_cube, (1, 2, 0))
    oriented = jnp.where(side_bit == 0, forward, backward)
    own_rows = lax.dynamic_slice_in_dim(oriented, column * piece_width, piece_width, 1)
    gram_piece = jnp.einsum("brc,bqc->brq", oriented, own_rows, preferred_element_type=jnp.float32)
    fresh_stat = statistics[:, 0] + gram_piece
    identity = jnp.eye(order_size, dtype=jnp.float32)

    def widen(values):
        return doubling(
            values, levels, device, 2, lambda portion, level_bit: swapped(portion, "tok", level_bit)
        )

    assembled = widen(fresh_stat)
    scaling = (2.5 / jnp.sqrt(jnp.sum(assembled * assembled, axis=(1, 2)) + 1e-06))[:, None, None]
    matrix = scaling * assembled
    factor = (5.0 * identity - matrix) * 0.25
    iterate = jnp.sqrt(jnp.sqrt(scaling)) * columns_of(factor)
    for repeat in range(1, ITERS):
        square = widen(product(factor, columns_of(factor)))
        fourth = widen(product(square, columns_of(square)))
        matrix = widen(product(fourth, columns_of(matrix)))
        factor = (5.0 * identity - matrix) * 0.25
        iterate = product(factor, iterate)
    own_root = doubling(
        iterate.astype(jnp.bfloat16),
        levels,
        device,
        2,
        lambda portion, level_bit: jax.tree.map(
            lambda part, own: part.astype(own.dtype),
            swapped(as_sent(portion), "tok", level_bit),
            portion,
        ),
    )
    other_root = swapped(own_root, "tok", levels)
    left_root = jnp.where(side_bit == 0, own_root, other_root)
    right_root = jnp.where(side_bit == 0, other_root, own_root)
    left_rows = lax.dynamic_slice_in_dim(left_root, slab_index * rows_dev, rows_dev, 1)
    mixed_rows = jnp.einsum(
        "bsr,rbc->bsc", left_rows, grad_cube, preferred_element_type=jnp.float32
    ).astype(jnp.bfloat16)
    update = jnp.einsum(
        "bsc,bcd->sbd", mixed_rows, right_root, preferred_element_type=jnp.float32
    ) * math.sqrt(order_size)
    return (update.reshape(rows_dev, blocks * order_size).astype(jnp.bfloat16), fresh_stat[:, None])


def product_of(left_side, right_side):
    return jnp.dot(left_side, right_side, preferred_element_type=jnp.float32)


def multiplied(left_side, right_side):
    return jnp.einsum(
        "bij,bjk->bik", left_side, right_side, preferred_element_type=jnp.float32
    )


def rounded(values):
    return lax.optimization_barrier(values.astype(jnp.bfloat16))


def widened(values):
    return values.astype(jnp.float32)


def block_gradient(tokens, grads_out, blocks):
    count = lax.axis_size("tok")
    device = lax.axis_index("tok")
    groups = count // 2
    group, core = device // 2, device % 2
    rows_dev = tokens.shape[1] // count
    width = grads_out.shape[1] // blocks
    pair = [(d, d ^ 1) for d in range(count)]

    tokens_of = [tokens] * blocks

    def part(source, target, owner, block):
        rows = lax.dynamic_slice_in_dim(source, (target * 2 + owner) * rows_dev, rows_dev, 1)
        return lax.dot_general(
            rows,
            grads_out[:, block * width : (block + 1) * width],
            (((0,), (0,)), ((), ())),
            preferred_element_type=jnp.float32,
        )

    arriving = [None] * blocks
    for step in range(groups):
        for block in range(blocks):
            sign = 1 if block % 2 == 0 else -1
            target = (group - sign * (1 + step) + 2 * groups) % groups
            theirs = lax.ppermute(
                part(tokens_of[block], target, 1 - core, block).astype(jnp.bfloat16), "tok", pair
            )
            total = part(tokens_of[block], target, core, block) + theirs.astype(jnp.float32)
            if step < groups - 1 and step > 0:
                total = lax.optimization_barrier(total)
            if arriving[block] is not None:
                total = total + arriving[block].astype(jnp.float32)
            total, tokens_of[block] = lax.optimization_barrier((total.astype(jnp.bfloat16), tokens))
            if step < groups - 1:
                route = [(d, (d + sign * 2) % count) for d in range(count)]
                total = lax.ppermute(total, "tok", route)
            arriving[block] = total
    return arriving, core, pair


def on_device(tokens, grads_out, statistics):
    blocks, _, order_size, piece_width = statistics.shape
    if piece_width != order_size:
        return in_pieces(tokens, grads_out, statistics)
    rows_dev = tokens.shape[1] // lax.axis_size("tok")
    owned, core, pair = block_gradient(tokens, grads_out, blocks)
    partner = [lax.ppermute(half, "tok", pair) for half in owned]
    first_side = core == 0
    grad_cube = jnp.stack(
        [
            jnp.concatenate(
                [jnp.where(first_side, mine, other), jnp.where(first_side, other, mine)], 0
            )
            for mine, other in zip(owned, partner)
        ]
    )
    fresh_stat = lax.cond(
        first_side,
        lambda g, old: old
        + jnp.einsum("brc,bqc->brq", g, g, preferred_element_type=jnp.float32),
        lambda g, old: old
        + jnp.einsum("brc,brq->bcq", g, g, preferred_element_type=jnp.float32),
        grad_cube,
        statistics[:, 0],
    )
    identity = jnp.eye(order_size, dtype=jnp.float32)
    scaling = (2.5 / jnp.sqrt(jnp.sum(fresh_stat * fresh_stat, axis=(1, 2)) + 1e-06))[:, None, None]
    matrix = rounded(scaling * fresh_stat)
    unit = 1.25
    rest = None
    for repeat in range(1, ITERS):
        square = rounded(
            multiplied(matrix, matrix) * 0.0625 - 0.625 * widened(matrix) + 1.5625 * identity
        )
        fourth = rounded(multiplied(square, square))
        before, matrix = matrix, rounded(multiplied(fourth, matrix))
        if rest is None:
            grown = (
                multiplied(matrix, before) * 0.0625
                - (0.25 * 1.25) * (widened(before) + widened(matrix))
            )
        else:
            last = repeat == ITERS - 1
            grown = [
                1.25 * widened(r) - (0.25 * unit) * widened(m) - 0.25 * product_of(m, r)
                for m, r in ((matrix[i], rest[i]) for i in range(blocks))
            ]
            if not last:
                grown = jnp.stack(grown)
        unit = 1.25 * unit
        if repeat < ITERS - 1:
            rest = rounded(grown)
    gain = jnp.sqrt(jnp.sqrt(scaling))
    own_root = [
        lax.optimization_barrier((gain[i] * (unit * identity + grown[i])).astype(jnp.bfloat16))
        for i in range(blocks)
    ]
    other_root = [lax.ppermute(root, "tok", pair) for root in own_root]
    update = []
    for i in range(blocks):
        right_root = jnp.where(first_side, other_root[i], own_root[i])
        left_rows = jnp.where(
            first_side,
            lax.dynamic_slice_in_dim(own_root[i], core * rows_dev, rows_dev, 0),
            lax.dynamic_slice_in_dim(other_root[i], core * rows_dev, rows_dev, 0),
        )
        mixed_rows = rounded(product_of(left_rows, grad_cube[i]))
        step = product_of(mixed_rows, right_root) * math.sqrt(order_size)
        update.append(step.astype(jnp.bfloat16))
    return (jnp.concatenate(update, 1), fresh_stat[:, None])


def solution(mesh):
    placed = (P("tok", None), P("tok", "col"), P("col", "tok", None, None))
    return jax.shard_map(
        on_device,
        mesh=mesh,
        in_specs=placed,
        out_specs=(P("tok", "col"), P("col", "tok", None, None)),
        check_vma=False,
    )
```
